32 devices in a mesh: pts: 8 (over z, y), grp: 4 (over x, core).
Axes of the slice: x: 2, y: 2, z: 4, core: 2. Of those that a mesh axis runs over, the one named last changes fastest.
Arguments:
- jacobian: bfloat16 [4096, 3, 3, 384], P(('pts', 'grp')), may hold values from -0.15625 to 0.15625
- owner: int32 [4096, 1], P(('pts', 'grp')), may hold values from 0 to 7; in each aligned block of 128 rows (0 to 127, 128 to 255, ...) at most 32 rows name the same one
- damping: float32 [8, 384], P('pts'), may hold values from 0.2 to 2
Outputs:
- reduced_diag: float32 [8, 384, 384], P('pts', None, 'grp')
- reduced_pair: float32 [8, 384, 384], P('pts', None, 'grp')
The draws below stay inside these ranges and needn't reach their ends.
Inputs may be any that keep to these rules, and one draw needn't show every extreme that they name: `owner`: among the 128 landmarks of one device at most 32 name the same segment, and in every draw some segment is named by exactly 32 landmarks of some device.
All inputs are finite; a program needn't handle non-finite values.
Results may differ from the reference program's by a relative error of at most 0.0003.
Values may be sent and summed in bfloat16 or wider, within the bound.
A program may use at most 64 MiB of HBM per device.

```python
import math
import jax
import jax.numpy as jnp
import numpy as np
from jax import lax

F = 384
PT = 128
CAP = 32
NE = 8
NPOINTS = 4096
N_PTS = 8
N_GRP = 4


def level_of(key, dims, cuts, low, top_value):
    def one(position, parts):
        steps = jax.random.uniform(jax.random.fold_in(jax.random.fold_in(key, 6), position), (parts,), jnp.float32, low / len(cuts), top_value / len(cuts))
        return jnp.repeat(jnp.exp(steps), dims[position] // parts).reshape((-1,) + (1,) * (len(dims) - position - 1))

    factor_of = one(*cuts[0])
    for cut in cuts[1:]:
        factor_of = factor_of * one(*cut)
    return factor_of


def assign_block(own_key, own, number, rows, amount, top, most, slope):
    order = jax.random.permutation(own_key, amount)
    heavy_load, usual = portions_of(amount, rows * top, most, slope, True), portions_of(amount, rows * top, most, slope, False)
    places = jnp.arange(amount)

    def named(sizes, offset_by):
        used = int((sizes > 0).sum())
        fixed = max(1, used // 4)
        moved = fixed + (places - fixed + offset_by * (used - fixed)) % max(1, amount - fixed)
        return jnp.zeros((amount,), jnp.int32).at[order[jnp.where(places < fixed, places, moved)]].set(jnp.asarray(sizes, jnp.int32))

    sizes = jnp.where(number % 4 == 0, named(heavy_load, number // 4), named(usual, number - number // 4 - 1))
    mixed = jax.random.permutation(jax.random.fold_in(own, 3), amount)
    source_of, sink = mixed[0:amount // 2 * 2:2], mixed[1:amount // 2 * 2:2]
    margin = jnp.minimum(sizes[source_of] - 1, most - sizes[sink]) // 2
    margin = jnp.where((source_of == order[0]) | (sink == order[0]) | (sizes[sink] == 0), 0, jnp.maximum(margin, 0))
    moved = jax.random.randint(jax.random.fold_in(own, 4), (amount // 2,), 0, 1 << 20) % (margin + 1)
    sizes = sizes.at[source_of].add(-moved).at[sink].add(moved)
    items = jnp.searchsorted(jnp.cumsum(sizes), jnp.arange(rows * top), side="right").astype(jnp.int32)
    table = items.reshape(top, rows).T
    table = table[jax.random.permutation(jax.random.fold_in(own, 1), rows)]
    offset_by = jax.random.randint(jax.random.fold_in(own, 2), (rows, 1), 0, top)
    return jnp.take_along_axis(table, (jnp.arange(top)[None, :] + offset_by) % top, axis=1)


def portions_of(amount, total, limit, slope, full):
    weights = [(1 << 20) // math.isqrt(grade ** slope) + 1 for grade in range(1, amount + 1)]
    largest = limit if full else min(limit, max(-(-total // amount), total * weights[0] // sum(weights)))
    least = 1 if total - largest >= amount - 1 else 0
    given, rest = [largest] + [least] * (amount - 1), total - largest - least * (amount - 1)
    while rest > 0:
        movable = [i for i in range(1, amount) if given[i] < largest] or [i for i in range(1, amount) if given[i] < limit]
        mass, budget = sum([weights[i] for i in movable]), rest
        for i in movable:
            extra = min(limit - given[i], max(1, budget * weights[i] // mass), rest)
            given[i] = given[i] + extra
            rest = rest - extra
    return np.array(given)


def bell_draw(rng, dims, spread, bound, split=(), held_as=jnp.bfloat16):
    values = jax.random.normal(rng, dims, jnp.float32) * spread
    if len(split) > 0:
        values = level_of(rng, dims, split, -0.22, 0.18) * values
    return jnp.clip(values, min=-bound, max=bound).astype(held_as)


def setup_inputs(seed: int = 0) -> dict:
    splits = jax.random.split(jax.random.key(seed), 4)
    jacobian = bell_draw(splits[0], (NPOINTS, 3, 3, F), (12 * PT) ** -0.5, 0.15625, ((0, 32),))
    owner_keys = jax.random.split(jax.random.fold_in(splits[1], 1), NPOINTS // PT)
    owner_turns = jax.random.permutation(jax.random.fold_in(splits[1], 3), NPOINTS // PT)
    owner = jax.vmap(lambda own, number: assign_block(jax.random.fold_in(splits[1], 2), own, number, PT, N_PTS, 1, CAP, 2))(owner_keys, owner_turns).reshape((NPOINTS, 1))
    damping = jnp.clip(jnp.exp(math.log(2.0) - 2.3025851 * jax.random.uniform(splits[2], (NE, F), jnp.float32) ** level_of(splits[2], (NE, F), ((0, 8),), -0.2, 0.2)), 0.2, 2.0)
    return {"jacobian": jacobian, "owner": owner, "damping": damping}


def gram(left, right):
    return lax.dot_general(left.astype(jnp.float32), right.astype(jnp.float32), (((0,), (0,)), ((), ())), preferred_element_type=jnp.float32)

def exact_gram(left, right):
    return lax.dot_general(left.astype(jnp.float32), right.astype(jnp.float32), (((0,), (0,)), ((), ())), precision=lax.Precision.HIGHEST, preferred_element_type=jnp.float32)

def reference(jacobian, owner, damping):
    window = N_PTS * N_GRP * CAP
    width = jacobian.shape[3]
    segment = owner[:, 0].astype(jnp.int32)
    order = jnp.argsort(segment, stable=True)
    sorted_rows = jacobian[order]
    counts = jax.ops.segment_sum(jnp.ones_like(segment), segment, num_segments=NE).astype(jnp.int32)
    starts = (jnp.cumsum(counts) - counts).astype(jnp.int32)
    padded = jnp.concatenate([sorted_rows, jnp.zeros((window, 3, 3, width), jacobian.dtype)], 0)

    def one_segment(items):
        start, count, lm_row = items
        rows = lax.dynamic_slice_in_dim(padded, start.astype(jnp.int32), window, 0)
        keep = jnp.arange(window, dtype=jnp.int32) < count
        rows = jnp.where(keep[:, None, None, None], rows, jnp.zeros_like(rows))
        first = rows[:, 0].reshape(window * 3, width)
        middle = rows[:, 1].reshape(window * 3, width)
        last = rows[:, 2].reshape(window * 3, width)
        d_low = gram(first, first)
        d_odd = gram(middle, middle)
        d_high = gram(last, last)
        b_low = gram(middle, first)
        b_high = gram(middle, last)
        e_pair = gram(first, last)
        system = d_odd + jnp.diag(lm_row)
        factor = jnp.linalg.cholesky(system)
        y_low = lax.linalg.triangular_solve(factor, b_low, left_side=True, lower=True)
        y_high = lax.linalg.triangular_solve(factor, b_high, left_side=True, lower=True)
        low = d_low - exact_gram(y_low, y_low)
        high = d_high - exact_gram(y_high, y_high)
        pair = e_pair - exact_gram(y_low, y_high)
        return (low, high, pair)
    low, high, pair = lax.map(one_segment, (starts, counts, damping))
    reduced_diag = low + jnp.roll(high, 1, axis=0)
    return (reduced_diag, pair)
```

```python
import functools

import jax
import jax.numpy as jnp
from jax import lax
from jax.experimental import pallas as pl
from jax.experimental.pallas import tpu as pltpu
from jax.sharding import PartitionSpec as P

MESH = pl.DeviceIdType.MESH
LANES = 128
TILE = 8


def mm(left, right, dims, precise):
    return lax.dot_general(
        left,
        right,
        (dims, ((), ())),
        precision=lax.Precision.HIGHEST if precise else None,
        preferred_element_type=jnp.float32,
    )


NN = ((1,), (0,))
NT = ((1,), (1,))
TN = ((0,), (0,))


def sweep_steps(matrix, rounds):
    size = matrix.shape[0]
    lane_row = lax.broadcasted_iota(jnp.int32, (1, size), 1)
    lane = lax.broadcasted_iota(jnp.int32, (size, size), 1)
    top_row = lax.broadcasted_iota(jnp.int32, (TILE, size), 0)

    def body(_, a):
        for t in range(TILE):
            row = a[t : t + 1, :]
            col = a[:, t : t + 1]
            scaled = jnp.where(lane_row == t, -1.0, row) * (1.0 / a[t : t + 1, t : t + 1])
            new = jnp.where(lane == t, 0.0, a) - col * scaled
            top = jnp.where(top_row == t, scaled, new[:TILE])
            a = jnp.concatenate([top, new[TILE:]], 0)
        a = pltpu.roll(a, size - TILE, 1)
        return jnp.concatenate([a[TILE:], a[:TILE]], 0)

    return lax.fori_loop(0, rounds, body, matrix)


def kernel(
    owners, groups, rows_per, width,
    send, damp, diag_out, pair_out,
    recv, sblk, s1, s2, gram, r1, r2, bt, highs, carried,
    a_send, a_recv, d_send, d_recv, d2_recv, g_send, g_recv, b_send, b_recv, c_send, c_recv, own_sem,
):
    me = lax.axis_index("pts")
    grp = lax.axis_index("grp")
    near = grp + 1 - 2 * lax.rem(grp, 2)
    far = lax.rem(grp + 2, groups)
    chunk = width // groups
    nb = width // LANES
    pairs = [(i, j) for i in range(nb) for j in range(i, nb)]
    odd = lax.rem(grp, 2)

    barrier = pltpu.get_barrier_semaphore()

    def greet(off, _):
        pl.semaphore_signal(
            barrier, inc=1, device_id=(lax.rem(me + off, owners), grp), device_id_type=MESH
        )
        return 0

    lax.fori_loop(1, owners, greet, 0)
    for other in (near, far):
        pl.semaphore_signal(barrier, inc=1, device_id=(me, other), device_id_type=MESH)
    pl.semaphore_wait(barrier, owners - 1 + 2)

    def rows_at(i):
        return pl.ds(pl.multiple_of(i * rows_per, rows_per), rows_per)

    for k in (1, 0, 2):
        def issue(off, _, k=k):
            to = lax.rem(me + off, owners)
            pltpu.make_async_remote_copy(
                src_ref=send.at[k, rows_at(to)],
                dst_ref=recv.at[k, rows_at(me)],
                send_sem=a_send.at[k],
                recv_sem=a_recv.at[k],
                device_id=(to, grp),
                device_id_type=MESH,
            ).start()
            return 0

        lax.fori_loop(1, owners, issue, 0)
    for k in range(3):
        pltpu.make_async_copy(
            send.at[k, rows_at(me)], recv.at[k, rows_at(me)], own_sem.at[k]
        ).start()
    for k in range(3):
        pltpu.make_async_copy(
            send.at[k, rows_at(me)], recv.at[k, rows_at(me)], own_sem.at[k]
        ).wait()

    def await_rows(k):
        part = recv.at[k, pl.ds(0, (owners - 1) * rows_per)]
        pltpu.make_async_copy(part, part, a_recv.at[k]).wait()

    await_rows(1)
    first_copies = []
    for n, (i, j) in enumerate(pairs):
        sblk[n] = mm(
            recv[1, :, i * LANES : (i + 1) * LANES],
            recv[1, :, j * LANES : (j + 1) * LANES], TN, False,
        )
        copy = pltpu.make_async_remote_copy(
            src_ref=sblk.at[n], dst_ref=s1.at[n],
            send_sem=d_send.at[n], recv_sem=d_recv.at[n],
            device_id=(me, near), device_id_type=MESH,
        )
        copy.start()
        first_copies.append(copy)
    second_copies = []
    own = len(pairs)
    for n in range(own):
        first_copies[n].wait_recv()
        sblk[own + n] = sblk[n] + s1[n]
        copy = pltpu.make_async_remote_copy(
            src_ref=sblk.at[own + n], dst_ref=s2.at[n],
            send_sem=d_send.at[own + n], recv_sem=d2_recv.at[n],
            device_id=(me, far), device_id_type=MESH,
        )
        copy.start()
        second_copies.append(copy)

    eye = (
        lax.broadcasted_iota(jnp.int32, (LANES, LANES), 0)
        == lax.broadcasted_iota(jnp.int32, (LANES, LANES), 1)
    )

    def reduced(n):
        second_copies[n].wait_recv()
        i, j = pairs[n]
        total = sblk[own + n] + s2[n]
        if i == j:
            total = total + jnp.where(eye, damp[:, i * LANES : (i + 1) * LANES], 0.0)
        return total

    where_in = {pair: n for n, pair in enumerate(pairs)}
    blocks = {}
    inverses, factors = [], {}
    rounds = LANES // TILE
    half = rounds // 2

    sides = ((0, 1), (2, 1), (0, 0), (2, 2), (2, 0))
    count = len(sides)

    def chunk_rows(c):
        return pl.ds(pl.multiple_of(c * chunk, TILE), chunk)

    def make_grams():
        await_rows(0)
        await_rows(2)
        for m, (left, right) in enumerate(sides):
            gram[m] = mm(recv[left], recv[right], TN, False)
            for h in range(2):
                near_copy(m, h).start()

    def near_copy(m, h):
        return pltpu.make_async_remote_copy(
            src_ref=gram.at[m, chunk_rows(1 - odd + 2 * h)], dst_ref=r1.at[m, h],
            send_sem=g_send.at[m, h], recv_sem=g_recv.at[m, h],
            device_id=(me, near), device_id_type=MESH,
        )

    def far_copy(m):
        return pltpu.make_async_remote_copy(
            src_ref=gram.at[m, chunk_rows(far)], dst_ref=r2.at[m],
            send_sem=g_send.at[m, 2], recv_sem=g_recv.at[m, 2],
            device_id=(me, far), device_id_type=MESH,
        )

    def fold_near():
        for m in range(count):
            for h in range(2):
                near_copy(m, h).wait()
                at = chunk_rows(odd + 2 * h)
                gram[m, at, :] = gram[m, at, :] + r1[m, h]
            far_copy(m).start()

    def spread_far(m):
        return pltpu.make_async_remote_copy(
            src_ref=bt.at[m, chunk_rows(grp)], dst_ref=bt.at[m, chunk_rows(grp)],
            send_sem=b_send.at[m, 0], recv_sem=b_recv.at[m, 0],
            device_id=(me, far), device_id_type=MESH,
        )

    def spread_near(m, h):
        at = chunk_rows(odd + 2 * h)
        return pltpu.make_async_remote_copy(
            src_ref=bt.at[m, at], dst_ref=bt.at[m, at],
            send_sem=b_send.at[m, 1 + h], recv_sem=b_recv.at[m, 1 + h],
            device_id=(me, near), device_id_type=MESH,
        )

    def fold_far():
        for m in range(count):
            far_copy(m).wait()
            at = chunk_rows(grp)
            if m < 2:
                bt[m, at, :] = gram[m, at, :] + r2[m]
                spread_far(m).start()
            else:
                gram[m, at, :] = gram[m, at, :] + r2[m]

    def spread():
        for m in range(2):
            spread_far(m).wait()
            for h in range(2):
                spread_near(m, h).start()

    hooks = {(0, 1): make_grams, (1, 0): fold_near, (1, 1): fold_far, (2, 0): spread}
    for i in range(nb):
        for j in range(i, nb):
            blocks[i, j] = blocks[i, j] if i > 0 else reduced(where_in[i, j])
        if i == 0:
            for pair in pairs:
                if pair[0] > 0:
                    blocks[pair] = None
        a = sweep_steps(blocks[i, i], half)
        if (i, 0) in hooks:
            hooks.pop((i, 0))()
        a = -sweep_steps(a, rounds - half)
        if (i, 1) in hooks:
            hooks.pop((i, 1))()
        inverses.append(a)
        for j in range(i + 1, nb):
            factors[i, j] = mm(a, blocks[i, j], NN, True)
        for j in range(i + 1, nb):
            for k in range(j, nb):
                base = blocks[j, k]
                if base is None:
                    base = reduced(where_in[j, k])
                blocks[j, k] = base - mm(blocks[i, j], factors[i, k], TN, True)
    for key in sorted(hooks):
        hooks[key]()
    for m in range(2):
        for h in range(2):
            spread_near(m, h).wait()

    for m in range(2):
        for j in range(1, nb):
            value = bt[m, :, j * LANES : (j + 1) * LANES]
            for i in range(j):
                value = value - mm(
                    bt[m, :, i * LANES : (i + 1) * LANES], factors[i, j], NN, True
                )
            bt[m, :, j * LANES : (j + 1) * LANES] = value
    mine = chunk_rows(grp)
    solved = []
    for m in range(2):
        solved.append(
            jnp.concatenate(
                [
                    mm(bt[m, mine, i * LANES : (i + 1) * LANES], inverses[i], NN, True)
                    for i in range(nb)
                ],
                1,
            )
        )
    highs[...] = gram[3, mine, :] - mm(solved[1], bt[1], NT, True)
    carry = pltpu.make_async_remote_copy(
        src_ref=highs, dst_ref=carried, send_sem=c_send, recv_sem=c_recv,
        device_id=(lax.rem(me + 1, owners), grp), device_id_type=MESH,
    )
    carry.start()
    low = gram[2, mine, :] - mm(solved[0], bt[0], NT, True)
    pair_out[...] = (gram[4, mine, :] - mm(solved[1], bt[0], NT, True)).T
    for copy in first_copies + second_copies:
        copy.wait_send()
    for k in range(3):
        part = send.at[k, pl.ds(0, (owners - 1) * rows_per)]
        pltpu.make_async_copy(part, part, a_send.at[k]).wait()
    carry.wait()
    diag_out[...] = (low + carried[...]).T


def local(jacobian, owner, damping):
    points, clusters, residuals, width = jacobian.shape
    owners = lax.axis_size("pts")
    groups = lax.axis_size("grp")
    capacity = max(2, 2 * points // owners)
    rows_per = -(-residuals * capacity // 16) * 16
    total = owners * rows_per
    segment = owner[:, 0]
    same = segment[:, None] == segment[None, :]
    before = jnp.arange(points)[:, None] < jnp.arange(points)[None, :]
    rank = jnp.sum((same & before).astype(jnp.int32), axis=0)
    place = segment * rows_per + rank
    place = (place[None, :] + capacity * jnp.arange(residuals)[:, None]).reshape(-1)
    pick = (jnp.arange(total)[:, None] == place[None, :]).astype(jacobian.dtype)
    planes = jnp.transpose(jacobian, (1, 2, 0, 3)).reshape(clusters, residuals * points, width)
    outgoing = jnp.einsum(
        "qp,kpf->kqf", pick, planes, preferred_element_type=jnp.float32
    ).astype(jacobian.dtype)
    chunk = width // groups
    nb = width // LANES
    blocks = nb * (nb + 1) // 2
    vmem = pl.BlockSpec(memory_space=pltpu.VMEM)
    dma = pltpu.SemaphoreType.DMA
    diag, pair = pl.pallas_call(
        functools.partial(kernel, owners, groups, rows_per, width),
        out_shape=[jax.ShapeDtypeStruct((width, chunk), jnp.float32)] * 2,
        in_specs=[vmem, vmem],
        out_specs=[vmem, vmem],
        scratch_shapes=[
            pltpu.VMEM((clusters, total, width), jacobian.dtype),
            pltpu.VMEM((2 * blocks, LANES, LANES), jnp.float32),
            pltpu.VMEM((blocks, LANES, LANES), jnp.float32),
            pltpu.VMEM((blocks, LANES, LANES), jnp.float32),
            pltpu.VMEM((5, width, width), jnp.float32),
            pltpu.VMEM((5, 2, chunk, width), jnp.float32),
            pltpu.VMEM((5, chunk, width), jnp.float32),
            pltpu.VMEM((2, width, width), jnp.float32),
            pltpu.VMEM((chunk, width), jnp.float32),
            pltpu.VMEM((chunk, width), jnp.float32),
            dma((3,)), dma((3,)),
            dma((2 * blocks,)), dma((blocks,)), dma((blocks,)),
            dma((5, 3)), dma((5, 3)),
            dma((2, 3)), dma((2, 3)),
            dma, dma, dma((3,)),
        ],
        compiler_params=pltpu.CompilerParams(collective_id=0, has_side_effects=True),
    )(outgoing, damping)
    return diag[None], pair[None]


def solution(mesh):
    placed = (P(("pts", "grp"), None, None, None), P(("pts", "grp"), None), P("pts", None))
    return jax.shard_map(
        local,
        mesh=mesh,
        in_specs=placed,
        out_specs=(P("pts", None, "grp"), P("pts", None, "grp")),
        check_vma=False,
    )
```

```python
import functools

import jax
import jax.numpy as jnp
from jax import lax
from jax.experimental import pallas as pl
from jax.experimental.pallas import tpu as pltpu
from jax.sharding import PartitionSpec as P

MESH = pl.DeviceIdType.MESH
LANES = 128
TILE = 8


def mm(left, right, dims, precise):
    return lax.dot_general(
        left,
        right,
        (dims, ((), ())),
        precision=lax.Precision.HIGHEST if precise else None,
        preferred_element_type=jnp.float32,
    )


NN = ((1,), (0,))
NT = ((1,), (1,))
TN = ((0,), (0,))


def sweep_steps(matrix, rounds):
    size = matrix.shape[0]
    lane_row = lax.broadcasted_iota(jnp.int32, (1, size), 1)
    lane = lax.broadcasted_iota(jnp.int32, (size, size), 1)
    top_row = lax.broadcasted_iota(jnp.int32, (TILE, size), 0)

    def body(_, a):
        for t in range(TILE):
            row = a[t : t + 1, :]
            col = a[:, t : t + 1]
            scaled = jnp.where(lane_row == t, -1.0, row) * (1.0 / a[t : t + 1, t : t + 1])
            new = jnp.where(lane == t, 0.0, a) - col * scaled
            top = jnp.where(top_row == t, scaled, new[:TILE])
            a = jnp.concatenate([top, new[TILE:]], 0)
        a = pltpu.roll(a, size - TILE, 1)
        return jnp.concatenate([a[TILE:], a[:TILE]], 0)

    return lax.fori_loop(0, rounds, body, matrix)


def kernel(
    owners, groups, rows_per, width,
    send, damp, diag_out, pair_out,
    recv, sblk, s1, s2, gram, r1, r2, bt, highs, carried,
    a_send, a_recv, d_send, d_recv, d2_recv, g_send, g_recv, b_send, b_recv, c_send, c_recv, own_sem,
):
    me = lax.axis_index("pts")
    grp = lax.axis_index("grp")
    near = grp + 1 - 2 * lax.rem(grp, 2)
    far = lax.rem(grp + 2, groups)
    chunk = width // groups
    nb = width // LANES
    pairs = [(i, j) for i in range(nb) for j in range(i, nb)]
    odd = lax.rem(grp, 2)

    barrier = pltpu.get_barrier_semaphore()

    def greet(off, _):
        pl.semaphore_signal(
            barrier, inc=1, device_id=(lax.rem(me + off, owners), grp), device_id_type=MESH
        )
        return 0

    lax.fori_loop(1, owners, greet, 0)
    for other in (near, far):
        pl.semaphore_signal(barrier, inc=1, device_id=(me, other), device_id_type=MESH)
    pl.semaphore_wait(barrier, owners - 1 + 2)

    def rows_at(i):
        return pl.ds(pl.multiple_of(i * rows_per, rows_per), rows_per)

    for k in (1, 0, 2):
        def issue(off, _, k=k):
            to = lax.rem(me + off, owners)
            pltpu.make_async_remote_copy(
                src_ref=send.at[k, rows_at(to)],
                dst_ref=recv.at[k, rows_at(me)],
                send_sem=a_send.at[k],
                recv_sem=a_recv.at[k],
                device_id=(to, grp),
                device_id_type=MESH,
            ).start()
            return 0

        lax.fori_loop(1, owners, issue, 0)
    for k in range(3):
        pltpu.make_async_copy(
            send.at[k, rows_at(me)], recv.at[k, rows_at(me)], own_sem.at[k]
        ).start()
    for k in range(3):
        pltpu.make_async_copy(
            send.at[k, rows_at(me)], recv.at[k, rows_at(me)], own_sem.at[k]
        ).wait()

    def await_rows(k):
        part = recv.at[k, pl.ds(0, (owners - 1) * rows_per)]
        pltpu.make_async_copy(part, part, a_recv.at[k]).wait()

    await_rows(1)
    first_copies = []
    for n, (i, j) in enumerate(pairs):
        sblk[n] = mm(
            recv[1, :, i * LANES : (i + 1) * LANES],
            recv[1, :, j * LANES : (j + 1) * LANES], TN, False,
        )
        copy = pltpu.make_async_remote_copy(
            src_ref=sblk.at[n], dst_ref=s1.at[n],
            send_sem=d_send.at[n], recv_sem=d_recv.at[n],
            device_id=(me, near), device_id_type=MESH,
        )
        copy.start()
        first_copies.append(copy)
    second_copies = []
    own = len(pairs)
    for n in range(own):
        first_copies[n].wait_recv()
        sblk[own + n] = sblk[n] + s1[n]
        copy = pltpu.make_async_remote_copy(
            src_ref=sblk.at[own + n], dst_ref=s2.at[n],
            send_sem=d_send.at[own + n], recv_sem=d2_recv.at[n],
            device_id=(me, far), device_id_type=MESH,
        )
        copy.start()
        second_copies.append(copy)

    eye = (
        lax.broadcasted_iota(jnp.int32, (LANES, LANES), 0)
        == lax.broadcasted_iota(jnp.int32, (LANES, LANES), 1)
    )

    def reduced(n):
        second_copies[n].wait_recv()
        i, j = pairs[n]
        total = sblk[own + n] + s2[n]
        if i == j:
            total = total + jnp.where(eye, damp[:, i * LANES : (i + 1) * LANES], 0.0)
        return total

    where_in = {pair: n for n, pair in enumerate(pairs)}
    blocks = {}
    inverses, factors = [], {}
    rounds = LANES // TILE
    half = rounds // 2

    sides = ((0, 1), (2, 1), (0, 0), (2, 2), (2, 0))

    def chunk_rows(c):
        return pl.ds(pl.multiple_of(c * chunk, TILE), chunk)

    def near_copy(m, h):
        return pltpu.make_async_remote_copy(
            src_ref=gram.at[m, chunk_rows(1 - odd + 2 * h)], dst_ref=r1.at[m, h],
            send_sem=g_send.at[m, h], recv_sem=g_recv.at[m, h],
            device_id=(me, near), device_id_type=MESH,
        )

    def far_copy(m, h):
        return pltpu.make_async_remote_copy(
            src_ref=gram.at[m, chunk_rows(odd + 2 * h if m < 2 else far)], dst_ref=r2.at[m, h],
            send_sem=g_send.at[m, 2 + h], recv_sem=g_recv.at[m, 2 + h],
            device_id=(me, far), device_id_type=MESH,
        )

    def spread_near(m, h):
        at = chunk_rows(odd + 2 * h)
        return pltpu.make_async_remote_copy(
            src_ref=bt.at[m, at], dst_ref=bt.at[m, at],
            send_sem=b_send.at[m, h], recv_sem=b_recv.at[m, h],
            device_id=(me, near), device_id_type=MESH,
        )

    def far_parts(m):
        return range(2) if m < 2 else range(1)

    def make_grams(k, some):
        await_rows(k)
        for m in some:
            left, right = sides[m]
            gram[m] = mm(recv[left], recv[right], TN, False)
            for h in range(2):
                near_copy(m, h).start()

    def fold_near(some):
        for m in some:
            for h in range(2):
                near_copy(m, h).wait()
                at = chunk_rows(odd + 2 * h)
                gram[m, at, :] = gram[m, at, :] + r1[m, h]
            for h in far_parts(m):
                far_copy(m, h).start()

    def fold_far(m):
        for h in far_parts(m):
            far_copy(m, h).wait()
            if m < 2:
                at = chunk_rows(odd + 2 * h)
                bt[m, at, :] = gram[m, at, :] + r2[m, h]
                spread_near(m, h).start()
            else:
                at = chunk_rows(grp)
                gram[m, at, :] = gram[m, at, :] + r2[m, h]

    def second_near():
        fold_near((1, 3, 4))
        fold_far(0)

    hooks = {
        (0, 1): functools.partial(make_grams, 0, (0, 2)),
        (1, 0): functools.partial(fold_near, (0, 2)),
        (1, 1): functools.partial(make_grams, 2, (1, 3, 4)),
        (2, 0): second_near,
    }

    def block(i, j):
        if (i, j) not in blocks:
            blocks[i, j] = reduced(where_in[i, j])
        return blocks[i, j]

    for i in range(nb):
        a = sweep_steps(block(i, i), half)
        if (i, 0) in hooks:
            hooks.pop((i, 0))()
        a = -sweep_steps(a, rounds - half)
        inverses.append(a)
        for j in range(i + 1, nb):
            factors[i, j] = mm(a, block(i, j), NN, True)
        if (i, 1) in hooks:
            hooks.pop((i, 1))()
        for j in range(i + 1, nb):
            for k in range(j, nb):
                blocks[j, k] = block(j, k) - mm(block(i, j), factors[i, k], TN, True)
    for key in sorted(hooks):
        hooks[key]()
    mine = chunk_rows(grp)

    def eliminate(m):
        for h in range(2):
            spread_near(m, h).wait()
        for j in range(1, nb):
            value = bt[m, :, j * LANES : (j + 1) * LANES]
            for i in range(j):
                value = value - mm(
                    bt[m, :, i * LANES : (i + 1) * LANES], factors[i, j], NN, True
                )
            bt[m, :, j * LANES : (j + 1) * LANES] = value
        return jnp.concatenate(
            [
                mm(bt[m, mine, i * LANES : (i + 1) * LANES], inverses[i], NN, True)
                for i in range(nb)
            ],
            1,
        )

    solved_low = eliminate(0)
    fold_far(1)
    fold_far(2)
    diag_out[...] = gram[2, mine, :] - mm(solved_low, bt[0], NT, True)
    solved_high = eliminate(1)
    fold_far(3)
    highs[...] = gram[3, mine, :] - mm(solved_high, bt[1], NT, True)
    carry = pltpu.make_async_remote_copy(
        src_ref=highs, dst_ref=carried, send_sem=c_send, recv_sem=c_recv,
        device_id=(lax.rem(me + 1, owners), grp), device_id_type=MESH,
    )
    carry.start()
    fold_far(4)
    pair_out[...] = gram[4, mine, :] - mm(solved_high, bt[0], NT, True)
    for copy in first_copies + second_copies:
        copy.wait_send()
    for k in range(3):
        part = send.at[k, pl.ds(0, (owners - 1) * rows_per)]
        pltpu.make_async_copy(part, part, a_send.at[k]).wait()
    carry.wait()
    diag_out[...] = diag_out[...] + carried[...]


def local(jacobian, owner, damping):
    points, clusters, residuals, width = jacobian.shape
    owners = lax.axis_size("pts")
    groups = lax.axis_size("grp")
    capacity = max(2, 2 * points // owners)
    rows_per = -(-residuals * capacity // 16) * 16
    total = owners * rows_per
    segment = owner[:, 0]
    same = segment[:, None] == segment[None, :]
    before = jnp.arange(points)[:, None] < jnp.arange(points)[None, :]
    rank = jnp.sum((same & before).astype(jnp.int32), axis=0)
    place = segment * rows_per + rank
    place = (place[None, :] + capacity * jnp.arange(residuals)[:, None]).reshape(-1)
    pick = (jnp.arange(total)[:, None] == place[None, :]).astype(jacobian.dtype)
    planes = jnp.transpose(jacobian, (1, 2, 0, 3)).reshape(clusters, residuals * points, width)
    outgoing = jnp.einsum(
        "qp,kpf->kqf", pick, planes, preferred_element_type=jnp.float32
    ).astype(jacobian.dtype)
    chunk = width // groups
    nb = width // LANES
    blocks = nb * (nb + 1) // 2
    vmem = pl.BlockSpec(memory_space=pltpu.VMEM)
    dma = pltpu.SemaphoreType.DMA
    diag, pair = pl.pallas_call(
        functools.partial(kernel, owners, groups, rows_per, width),
        out_shape=[jax.ShapeDtypeStruct((chunk, width), jnp.float32)] * 2,
        in_specs=[vmem, vmem],
        out_specs=[vmem, vmem],
        scratch_shapes=[
            pltpu.VMEM((clusters, total, width), jacobian.dtype),
            pltpu.VMEM((2 * blocks, LANES, LANES), jnp.float32),
            pltpu.VMEM((blocks, LANES, LANES), jnp.float32),
            pltpu.VMEM((blocks, LANES, LANES), jnp.float32),
            pltpu.VMEM((5, width, width), jnp.float32),
            pltpu.VMEM((5, 2, chunk, width), jnp.float32),
            pltpu.VMEM((5, 2, chunk, width), jnp.float32),
            pltpu.VMEM((2, width, width), jnp.float32),
            pltpu.VMEM((chunk, width), jnp.float32),
            pltpu.VMEM((chunk, width), jnp.float32),
            dma((3,)), dma((3,)),
            dma((2 * blocks,)), dma((blocks,)), dma((blocks,)),
            dma((5, 4)), dma((5, 4)),
            dma((2, 2)), dma((2, 2)),
            dma, dma, dma((3,)),
        ],
        compiler_params=pltpu.CompilerParams(collective_id=0, has_side_effects=True),
    )(outgoing, damping)
    return diag.T[None], pair.T[None]


def solution(mesh):
    placed = (P(("pts", "grp"), None, None, None), P(("pts", "grp"), None), P("pts", None))
    return jax.shard_map(
        local,
        mesh=mesh,
        in_specs=placed,
        out_specs=(P("pts", None, "grp"), P("pts", None, "grp")),
        check_vma=False,
    )
```

```python
import functools

import jax
import jax.numpy as jnp
from jax import lax
from jax.experimental import pallas as pl
from jax.experimental.pallas import tpu as pltpu
from jax.sharding import PartitionSpec as P

MESH = pl.DeviceIdType.MESH
LANES = 128
TILE = 8


def mm(left, right, dims, precise):
    return lax.dot_general(
        left,
        right,
        (dims, ((), ())),
        precision=lax.Precision.HIGHEST if precise else None,
        preferred_element_type=jnp.float32,
    )


NN = ((1,), (0,))
NT = ((1,), (1,))
TN = ((0,), (0,))


def sweep_steps(matrix, rounds):
    size = matrix.shape[0]
    lane_row = lax.broadcasted_iota(jnp.int32, (1, size), 1)
    lane = lax.broadcasted_iota(jnp.int32, (size, size), 1)
    top_row = lax.broadcasted_iota(jnp.int32, (TILE, size), 0)

    def body(_, a):
        for t in range(TILE):
            row = a[t : t + 1, :]
            col = a[:, t : t + 1]
            scaled = jnp.where(lane_row == t, -1.0, row) * (1.0 / a[t : t + 1, t : t + 1])
            new = jnp.where(lane == t, 0.0, a) - col * scaled
            top = jnp.where(top_row == t, scaled, new[:TILE])
            a = jnp.concatenate([top, new[TILE:]], 0)
        a = pltpu.roll(a, size - TILE, 1)
        return jnp.concatenate([a[TILE:], a[:TILE]], 0)

    return lax.fori_loop(0, rounds, body, matrix)


def kernel(
    owners, groups, rows_per, width, capacity,
    planes, owner_row, damp, low_out, pair_out, carried,
    send, recv, sblk, s1, s2, gram, r1, r2, bt, highs,
    a_send, a_recv, d_send, d_recv, d2_recv, g_send, g_recv, b_send, b_recv, c_send, c_recv, own_sem,
):
    me = lax.axis_index("pts")
    grp = lax.axis_index("grp")
    near = grp + 1 - 2 * lax.rem(grp, 2)
    far = lax.rem(grp + 2, groups)
    chunk = width // groups
    nb = width // LANES
    pairs = [(i, j) for i in range(nb) for j in range(i, nb)]
    odd = lax.rem(grp, 2)

    barrier = pltpu.get_barrier_semaphore()

    def greet(off, _):
        pl.semaphore_signal(
            barrier, inc=1, device_id=(lax.rem(me + off, owners), grp), device_id_type=MESH
        )
        return 0

    lax.fori_loop(1, owners, greet, 0)
    for other in (near, far):
        pl.semaphore_signal(barrier, inc=1, device_id=(me, other), device_id_type=MESH)

    clusters, spots, _ = planes.shape
    points = owner_row.shape[1]
    earlier = (
        lax.broadcasted_iota(jnp.int32, (points, points), 0)
        < lax.broadcasted_iota(jnp.int32, (points, points), 1)
    )
    spread = jnp.broadcast_to(owner_row[...], (points, points))
    ahead = jnp.where((spread.T == spread) & earlier, 1, 0)
    place = owner_row[...] * rows_per + jnp.sum(ahead, axis=0, keepdims=True)
    place = jnp.concatenate([place + capacity * r for r in range(spots // points)], 1)
    slot = lax.broadcasted_iota(jnp.int32, (owners * rows_per, spots), 0)
    pick = jnp.where(slot == place, 1.0, 0.0).astype(send.dtype)

    def pack(k):
        send[k] = mm(pick, planes[k], NN, False).astype(send.dtype)

    pack(1)
    pl.semaphore_wait(barrier, owners - 1 + 2)

    def rows_at(i):
        return pl.ds(pl.multiple_of(i * rows_per, rows_per), rows_per)

    for k in (1, 0, 2):
        if k != 1:
            pack(k)

        def issue(off, _, k=k):
            to = lax.rem(me + off, owners)
            pltpu.make_async_remote_copy(
                src_ref=send.at[k, rows_at(to)],
                dst_ref=recv.at[k, rows_at(me)],
                send_sem=a_send.at[k],
                recv_sem=a_recv.at[k],
                device_id=(to, grp),
                device_id_type=MESH,
            ).start()
            return 0

        lax.fori_loop(1, owners, issue, 0)
    for k in range(3):
        pltpu.make_async_copy(
            send.at[k, rows_at(me)], recv.at[k, rows_at(me)], own_sem.at[k]
        ).start()
    for k in range(3):
        pltpu.make_async_copy(
            send.at[k, rows_at(me)], recv.at[k, rows_at(me)], own_sem.at[k]
        ).wait()

    def await_rows(k):
        part = recv.at[k, pl.ds(0, (owners - 1) * rows_per)]
        pltpu.make_async_copy(part, part, a_recv.at[k]).wait()

    await_rows(1)
    first_copies = []
    own = len(pairs)
    for i in range(nb):
        strip = mm(
            recv[1, :, i * LANES : (i + 1) * LANES], recv[1, :, i * LANES :], TN, False
        )
        for j in range(i, nb):
            n = pairs.index((i, j))
            sblk[n] = strip[:, (j - i) * LANES : (j - i + 1) * LANES]
            copy = pltpu.make_async_remote_copy(
                src_ref=sblk.at[n], dst_ref=s1.at[n],
                send_sem=d_send.at[n], recv_sem=d_recv.at[n],
                device_id=(me, near), device_id_type=MESH,
            )
            copy.start()
            first_copies.append(copy)
    second_copies = []

    def forward(some):
        for n in some:
            first_copies[n].wait_recv()
            sblk[own + n] = sblk[n] + s1[n]
            copy = pltpu.make_async_remote_copy(
                src_ref=sblk.at[own + n], dst_ref=s2.at[n],
                send_sem=d_send.at[own + n], recv_sem=d2_recv.at[n],
                device_id=(me, far), device_id_type=MESH,
            )
            copy.start()
            second_copies.append(copy)

    forward(range(1))

    eye = (
        lax.broadcasted_iota(jnp.int32, (LANES, LANES), 0)
        == lax.broadcasted_iota(jnp.int32, (LANES, LANES), 1)
    )

    def reduced(n):
        second_copies[n].wait_recv()
        i, j = pairs[n]
        total = sblk[own + n] + s2[n]
        if i == j:
            total = total + jnp.where(eye, damp[:, i * LANES : (i + 1) * LANES], 0.0)
        return total

    where_in = {pair: n for n, pair in enumerate(pairs)}
    blocks = {}
    inverses, factors = [], {}
    rounds = LANES // TILE
    half = rounds // 2

    sides = ((0, 1), (2, 1), (0, 0), (2, 2), (2, 0))

    def chunk_rows(c):
        return pl.ds(pl.multiple_of(c * chunk, TILE), chunk)

    def near_copy(m, h):
        return pltpu.make_async_remote_copy(
            src_ref=gram.at[m, chunk_rows(1 - odd + 2 * h)], dst_ref=r1.at[m, h],
            send_sem=g_send.at[m, h], recv_sem=g_recv.at[m, h],
            device_id=(me, near), device_id_type=MESH,
        )

    def far_copy(m, h):
        return pltpu.make_async_remote_copy(
            src_ref=gram.at[m, chunk_rows(odd + 2 * h if m < 2 else far)], dst_ref=r2.at[m, h],
            send_sem=g_send.at[m, 2 + h], recv_sem=g_recv.at[m, 2 + h],
            device_id=(me, far), device_id_type=MESH,
        )

    def spread_near(m, h):
        at = chunk_rows(odd + 2 * h)
        return pltpu.make_async_remote_copy(
            src_ref=bt.at[m, at], dst_ref=bt.at[m, at],
            send_sem=b_send.at[m, h], recv_sem=b_recv.at[m, h],
            device_id=(me, near), device_id_type=MESH,
        )

    def far_parts(m):
        return range(2) if m < 2 else range(1)

    def make_grams(k, some):
        await_rows(k)
        for m in some:
            left, right = sides[m]
            gram[m] = mm(recv[left], recv[right], TN, False)
            for h in range(2):
                near_copy(m, h).start()

    def fold_near(some):
        for m in some:
            for h in range(2):
                near_copy(m, h).wait()
                at = chunk_rows(odd + 2 * h)
                gram[m, at, :] = gram[m, at, :] + r1[m, h]
            for h in far_parts(m):
                far_copy(m, h).start()

    def fold_far(m):
        for h in far_parts(m):
            far_copy(m, h).wait()
            if m < 2:
                at = chunk_rows(odd + 2 * h)
                bt[m, at, :] = gram[m, at, :] + r2[m, h]
                spread_near(m, h).start()
            else:
                at = chunk_rows(grp)
                gram[m, at, :] = gram[m, at, :] + r2[m, h]

    def second_near():
        fold_near((1, 3, 4))
        fold_far(0)

    hooks = {
        (0, 0): functools.partial(forward, range(1, own)),
        (0, 1): functools.partial(make_grams, 0, (0, 2)),
        (1, 0): functools.partial(fold_near, (0, 2)),
        (1, 1): functools.partial(make_grams, 2, (1, 3, 4)),
        (2, 0): second_near,
    }

    def block(i, j):
        if (i, j) not in blocks:
            blocks[i, j] = reduced(where_in[i, j])
        return blocks[i, j]

    for i in range(nb):
        head = half if i > 0 else half // 2
        a = sweep_steps(block(i, i), head)
        if (i, 0) in hooks:
            hooks.pop((i, 0))()
        a = -sweep_steps(a, rounds - head)
        inverses.append(a)
        for j in range(i + 1, nb):
            factors[i, j] = mm(a, block(i, j), NN, True)
        if (i, 1) in hooks:
            hooks.pop((i, 1))()
        for j in range(i + 1, nb):
            for k in range(j, nb):
                blocks[j, k] = block(j, k) - mm(block(i, j), factors[i, k], TN, True)
    for key in sorted(hooks):
        hooks[key]()
    mine = chunk_rows(grp)

    def eliminate(m):
        for h in range(2):
            spread_near(m, h).wait()
        for j in range(1, nb):
            value = bt[m, :, j * LANES : (j + 1) * LANES]
            for i in range(j):
                value = value - mm(
                    bt[m, :, i * LANES : (i + 1) * LANES], factors[i, j], NN, True
                )
            bt[m, :, j * LANES : (j + 1) * LANES] = value
        return jnp.concatenate(
            [
                mm(bt[m, mine, i * LANES : (i + 1) * LANES], inverses[i], NN, True)
                for i in range(nb)
            ],
            1,
        )

    solved_low = eliminate(0)
    fold_far(1)
    fold_far(2)
    low_out[...] = gram[2, mine, :] - mm(solved_low, bt[0], NT, True)
    solved_high = eliminate(1)
    fold_far(3)
    highs[...] = gram[3, mine, :] - mm(solved_high, bt[1], NT, True)
    carry = pltpu.make_async_remote_copy(
        src_ref=highs, dst_ref=carried, send_sem=c_send, recv_sem=c_recv,
        device_id=(lax.rem(me + 1, owners), grp), device_id_type=MESH,
    )
    carry.start()
    fold_far(4)
    pair_out[...] = gram[4, mine, :] - mm(solved_high, bt[0], NT, True)
    for copy in first_copies + second_copies:
        copy.wait_send()
    for k in range(3):
        part = send.at[k, pl.ds(0, (owners - 1) * rows_per)]
        pltpu.make_async_copy(part, part, a_send.at[k]).wait()
    carry.wait()


def finish(low, pair, carried, diag_out, pair_out):
    diag_out[...] = low[...] + carried[...]
    pair_out[...] = pair[...]


def local(jacobian, owner, damping):
    points, clusters, residuals, width = jacobian.shape
    owners = lax.axis_size("pts")
    groups = lax.axis_size("grp")
    capacity = max(2, 2 * points // owners)
    rows_per = -(-residuals * capacity // 16) * 16
    total = owners * rows_per
    planes = jnp.transpose(jacobian, (1, 2, 0, 3)).reshape(clusters, residuals * points, width)
    chunk = width // groups
    nb = width // LANES
    blocks = nb * (nb + 1) // 2
    vmem = pl.BlockSpec(memory_space=pltpu.VMEM)
    dma = pltpu.SemaphoreType.DMA
    low, pair, carried = pl.pallas_call(
        functools.partial(kernel, owners, groups, rows_per, width, capacity),
        out_shape=[jax.ShapeDtypeStruct((chunk, width), jnp.float32)] * 3,
        in_specs=[vmem] * 3,
        out_specs=[vmem] * 3,
        scratch_shapes=[
            pltpu.VMEM((clusters, total, width), jacobian.dtype),
            pltpu.VMEM((clusters, total, width), jacobian.dtype),
            pltpu.VMEM((2 * blocks, LANES, LANES), jnp.float32),
            pltpu.VMEM((blocks, LANES, LANES), jnp.float32),
            pltpu.VMEM((blocks, LANES, LANES), jnp.float32),
            pltpu.VMEM((5, width, width), jnp.float32),
            pltpu.VMEM((5, 2, chunk, width), jnp.float32),
            pltpu.VMEM((5, 2, chunk, width), jnp.float32),
            pltpu.VMEM((2, width, width), jnp.float32),
            pltpu.VMEM((chunk, width), jnp.float32),
            dma((3,)), dma((3,)),
            dma((2 * blocks,)), dma((blocks,)), dma((blocks,)),
            dma((5, 4)), dma((5, 4)),
            dma((2, 2)), dma((2, 2)),
            dma, dma, dma((3,)),
        ],
        compiler_params=pltpu.CompilerParams(collective_id=0, has_side_effects=True),
    )(planes, owner.reshape(1, points), damping)
    diag, pair = pl.pallas_call(
        finish,
        out_shape=[jax.ShapeDtypeStruct((chunk, width), jnp.float32)] * 2,
        in_specs=[vmem] * 3,
        out_specs=[vmem] * 2,
    )(low, pair, carried)
    return diag.T[None], pair.T[None]


def solution(mesh):
    placed = (P(("pts", "grp"), None, None, None), P(("pts", "grp"), None), P("pts", None))
    return jax.shard_map(
        local,
        mesh=mesh,
        in_specs=placed,
        out_specs=(P("pts", None, "grp"), P("pts", None, "grp")),
        check_vma=False,
    )
```

```python
import functools

import jax
import jax.numpy as jnp
from jax import lax
from jax.experimental import pallas as pl
from jax.experimental.pallas import tpu as pltpu
from jax.sharding import PartitionSpec as P

MESH = pl.DeviceIdType.MESH
LANES = 128
TILE = 8


def mm(left, right, dims, precise):
    return lax.dot_general(
        left,
        right,
        (dims, ((), ())),
        precision=lax.Precision.HIGHEST if precise else None,
        preferred_element_type=jnp.float32,
    )


NN = ((1,), (0,))
NT = ((1,), (1,))
TN = ((0,), (0,))


def sweep_steps(matrix, rounds):
    size = matrix.shape[0]
    lane_row = lax.broadcasted_iota(jnp.int32, (1, size), 1)
    lane = lax.broadcasted_iota(jnp.int32, (size, size), 1)
    top_row = lax.broadcasted_iota(jnp.int32, (TILE, size), 0)

    def body(_, a):
        for t in range(TILE):
            row = a[t : t + 1, :]
            col = a[:, t : t + 1]
            inverse = 1.0 / a[t : t + 1, t : t + 1]
            marked = jnp.where(lane_row == t, -1.0, row)
            new = jnp.where(lane == t, 0.0, a) - (col * marked) * inverse
            top = jnp.where(top_row == t, marked * inverse, new[:TILE])
            a = jnp.concatenate([top, new[TILE:]], 0)
        a = pltpu.roll(a, size - TILE, 1)
        return jnp.concatenate([a[TILE:], a[:TILE]], 0)

    return lax.fori_loop(0, rounds, body, matrix)


def kernel(
    owners, groups, rows_per, width, capacity,
    planes, owner_row, damp, low_out, pair_out, carried,
    send, recv, sblk, s1, s2, gram, r1, r2, bt, highs,
    a_send, a_recv, d_send, d_recv, d2_recv, g_send, g_recv, b_send, b_recv, c_send, c_recv, own_sem,
):
    me = lax.axis_index("pts")
    grp = lax.axis_index("grp")
    near = grp + 1 - 2 * lax.rem(grp, 2)
    far = lax.rem(grp + 2, groups)
    chunk = width // groups
    nb = width // LANES
    pairs = [(i, j) for i in range(nb) for j in range(i, nb)]
    odd = lax.rem(grp, 2)

    barrier = pltpu.get_barrier_semaphore()

    def greet(off, _):
        pl.semaphore_signal(
            barrier, inc=1, device_id=(lax.rem(me + off, owners), grp), device_id_type=MESH
        )
        return 0

    lax.fori_loop(1, owners, greet, 0)
    for other in (near, far):
        pl.semaphore_signal(barrier, inc=1, device_id=(me, other), device_id_type=MESH)

    clusters, spots, _ = planes.shape
    points = owner_row.shape[1]
    earlier = (
        lax.broadcasted_iota(jnp.int32, (points, points), 0)
        < lax.broadcasted_iota(jnp.int32, (points, points), 1)
    )
    spread = jnp.broadcast_to(owner_row[...], (points, points))
    ahead = jnp.where((spread.T == spread) & earlier, 1, 0)
    place = owner_row[...] * rows_per + jnp.sum(ahead, axis=0, keepdims=True)
    place = jnp.concatenate([place + capacity * r for r in range(spots // points)], 1)
    slot = lax.broadcasted_iota(jnp.int32, (owners * rows_per, spots), 0)
    pick = jnp.where(slot == place, 1.0, 0.0).astype(send.dtype)

    def pack(k):
        send[k] = mm(pick, planes[k], NN, False).astype(send.dtype)

    pack(1)
    pl.semaphore_wait(barrier, owners - 1 + 2)

    def rows_at(i):
        return pl.ds(pl.multiple_of(i * rows_per, rows_per), rows_per)

    for k in (1, 0, 2):
        if k != 1:
            pack(k)

        def issue(off, _, k=k):
            to = lax.rem(me + off, owners)
            pltpu.make_async_remote_copy(
                src_ref=send.at[k, rows_at(to)],
                dst_ref=recv.at[k, rows_at(me)],
                send_sem=a_send.at[k],
                recv_sem=a_recv.at[k],
                device_id=(to, grp),
                device_id_type=MESH,
            ).start()
            return 0

        lax.fori_loop(1, owners, issue, 0)
    for k in range(3):
        pltpu.make_async_copy(
            send.at[k, rows_at(me)], recv.at[k, rows_at(me)], own_sem.at[k]
        ).start()
    for k in range(3):
        pltpu.make_async_copy(
            send.at[k, rows_at(me)], recv.at[k, rows_at(me)], own_sem.at[k]
        ).wait()

    def await_rows(k):
        part = recv.at[k, pl.ds(0, (owners - 1) * rows_per)]
        pltpu.make_async_copy(part, part, a_recv.at[k]).wait()

    await_rows(1)
    first_copies = []
    own = len(pairs)
    for i in range(nb):
        strip = mm(
            recv[1, :, i * LANES : (i + 1) * LANES], recv[1, :, i * LANES :], TN, False
        )
        for j in range(i, nb):
            n = pairs.index((i, j))
            sblk[n] = strip[:, (j - i) * LANES : (j - i + 1) * LANES]
            copy = pltpu.make_async_remote_copy(
                src_ref=sblk.at[n], dst_ref=s1.at[n],
                send_sem=d_send.at[n], recv_sem=d_recv.at[n],
                device_id=(me, near), device_id_type=MESH,
            )
            copy.start()
            first_copies.append(copy)
    second_copies = []

    def forward(some):
        for n in some:
            first_copies[n].wait_recv()
            sblk[own + n] = sblk[n] + s1[n]
            copy = pltpu.make_async_remote_copy(
                src_ref=sblk.at[own + n], dst_ref=s2.at[n],
                send_sem=d_send.at[own + n], recv_sem=d2_recv.at[n],
                device_id=(me, far), device_id_type=MESH,
            )
            copy.start()
            second_copies.append(copy)

    forward(range(1))

    eye = (
        lax.broadcasted_iota(jnp.int32, (LANES, LANES), 0)
        == lax.broadcasted_iota(jnp.int32, (LANES, LANES), 1)
    )

    def reduced(n):
        second_copies[n].wait_recv()
        i, j = pairs[n]
        total = sblk[own + n] + s2[n]
        if i == j:
            total = total + jnp.where(eye, damp[:, i * LANES : (i + 1) * LANES], 0.0)
        return total

    where_in = {pair: n for n, pair in enumerate(pairs)}
    blocks = {}
    inverses, factors = [], {}
    rounds = LANES // TILE

    sides = ((0, 1), (2, 1), (0, 0), (2, 2), (2, 0))

    def chunk_rows(c):
        return pl.ds(pl.multiple_of(c * chunk, TILE), chunk)

    def near_copy(m, h):
        return pltpu.make_async_remote_copy(
            src_ref=gram.at[m, chunk_rows(1 - odd + 2 * h)], dst_ref=r1.at[m, h],
            send_sem=g_send.at[m, h], recv_sem=g_recv.at[m, h],
            device_id=(me, near), device_id_type=MESH,
        )

    def far_copy(m, h):
        return pltpu.make_async_remote_copy(
            src_ref=gram.at[m, chunk_rows(odd + 2 * h if m < 2 else far)], dst_ref=r2.at[m, h],
            send_sem=g_send.at[m, 2 + h], recv_sem=g_recv.at[m, 2 + h],
            device_id=(me, far), device_id_type=MESH,
        )

    def spread_near(m, h):
        at = chunk_rows(odd + 2 * h)
        return pltpu.make_async_remote_copy(
            src_ref=bt.at[m, at], dst_ref=bt.at[m, at],
            send_sem=b_send.at[m, h], recv_sem=b_recv.at[m, h],
            device_id=(me, near), device_id_type=MESH,
        )

    def far_parts(m):
        return range(2) if m < 2 else range(1)

    def make_grams(k, some):
        await_rows(k)
        for m in some:
            left, right = sides[m]
            gram[m] = mm(recv[left], recv[right], TN, False)
            for h in range(2):
                near_copy(m, h).start()

    def fold_near(some):
        for m in some:
            for h in range(2):
                near_copy(m, h).wait()
                at = chunk_rows(odd + 2 * h)
                gram[m, at, :] = gram[m, at, :] + r1[m, h]
            for h in far_parts(m):
                far_copy(m, h).start()

    def fold_far(m):
        for h in far_parts(m):
            far_copy(m, h).wait()
            if m < 2:
                at = chunk_rows(odd + 2 * h)
                bt[m, at, :] = gram[m, at, :] + r2[m, h]
                spread_near(m, h).start()
            else:
                at = chunk_rows(grp)
                gram[m, at, :] = gram[m, at, :] + r2[m, h]

    def second_near():
        fold_near((1,))
        fold_far(0)

    quarters = 4
    hooks = {
        (0, 1): functools.partial(forward, range(1, own)),
        (0, quarters): functools.partial(make_grams, 0, (0, 2)),
        (1, 1): functools.partial(fold_near, (0,)),
        (1, 2): functools.partial(fold_near, (2,)),
        (1, quarters): functools.partial(make_grams, 2, (1, 3, 4)),
        (2, 1): second_near,
        (2, 2): functools.partial(fold_near, (3,)),
        (2, 3): functools.partial(fold_near, (4,)),
    }

    def block(i, j):
        if (i, j) not in blocks:
            blocks[i, j] = reduced(where_in[i, j])
        return blocks[i, j]

    for i in range(nb):
        a = block(i, i)
        for part in range(1, quarters + 1):
            a = sweep_steps(a, rounds // quarters)
            if part < quarters and (i, part) in hooks:
                hooks.pop((i, part))()
        a = -a
        inverses.append(a)
        for j in range(i + 1, nb):
            factors[i, j] = mm(a, block(i, j), NN, True)
        if (i, quarters) in hooks:
            hooks.pop((i, quarters))()
        for j in range(i + 1, nb):
            for k in range(j, nb):
                blocks[j, k] = block(j, k) - mm(block(i, j), factors[i, k], TN, True)
    for key in sorted(hooks):
        hooks[key]()
    mine = chunk_rows(grp)

    def eliminate(m):
        for h in range(2):
            spread_near(m, h).wait()
        for j in range(1, nb):
            value = bt[m, :, j * LANES : (j + 1) * LANES]
            for i in range(j):
                value = value - mm(
                    bt[m, :, i * LANES : (i + 1) * LANES], factors[i, j], NN, True
                )
            bt[m, :, j * LANES : (j + 1) * LANES] = value
        return jnp.concatenate(
            [
                mm(bt[m, mine, i * LANES : (i + 1) * LANES], inverses[i], NN, True)
                for i in range(nb)
            ],
            1,
        )

    fold_far(1)
    solved_low = eliminate(0)
    fold_far(2)
    low_out[...] = gram[2, mine, :] - mm(solved_low, bt[0], NT, True)
    solved_high = eliminate(1)
    fold_far(3)
    highs[...] = gram[3, mine, :] - mm(solved_high, bt[1], NT, True)
    carry = pltpu.make_async_remote_copy(
        src_ref=highs, dst_ref=carried, send_sem=c_send, recv_sem=c_recv,
        device_id=(lax.rem(me + 1, owners), grp), device_id_type=MESH,
    )
    carry.start()
    fold_far(4)
    pair_out[...] = gram[4, mine, :] - mm(solved_high, bt[0], NT, True)
    for copy in first_copies + second_copies:
        copy.wait_send()
    for k in range(3):
        part = send.at[k, pl.ds(0, (owners - 1) * rows_per)]
        pltpu.make_async_copy(part, part, a_send.at[k]).wait()
    carry.wait()


def finish(low, pair, carried, diag_out, pair_out):
    diag_out[...] = low[...] + carried[...]
    pair_out[...] = pair[...]


def local(jacobian, owner, damping):
    points, clusters, residuals, width = jacobian.shape
    owners = lax.axis_size("pts")
    groups = lax.axis_size("grp")
    capacity = max(2, 2 * points // owners)
    rows_per = -(-residuals * capacity // 16) * 16
    total = owners * rows_per
    planes = jnp.transpose(jacobian, (1, 2, 0, 3)).reshape(clusters, residuals * points, width)
    chunk = width // groups
    nb = width // LANES
    blocks = nb * (nb + 1) // 2
    vmem = pl.BlockSpec(memory_space=pltpu.VMEM)
    dma = pltpu.SemaphoreType.DMA
    low, pair, carried = pl.pallas_call(
        functools.partial(kernel, owners, groups, rows_per, width, capacity),
        out_shape=[jax.ShapeDtypeStruct((chunk, width), jnp.float32)] * 3,
        in_specs=[vmem] * 3,
        out_specs=[vmem] * 3,
        scratch_shapes=[
            pltpu.VMEM((clusters, total, width), jacobian.dtype),
            pltpu.VMEM((clusters, total, width), jacobian.dtype),
            pltpu.VMEM((2 * blocks, LANES, LANES), jnp.float32),
            pltpu.VMEM((blocks, LANES, LANES), jnp.float32),
            pltpu.VMEM((blocks, LANES, LANES), jnp.float32),
            pltpu.VMEM((5, width, width), jnp.float32),
            pltpu.VMEM((5, 2, chunk, width), jnp.float32),
            pltpu.VMEM((5, 2, chunk, width), jnp.float32),
            pltpu.VMEM((2, width, width), jnp.float32),
            pltpu.VMEM((chunk, width), jnp.float32),
            dma((3,)), dma((3,)),
            dma((2 * blocks,)), dma((blocks,)), dma((blocks,)),
            dma((5, 4)), dma((5, 4)),
            dma((2, 2)), dma((2, 2)),
            dma, dma, dma((3,)),
        ],
        compiler_params=pltpu.CompilerParams(collective_id=0, has_side_effects=True),
    )(planes, owner.reshape(1, points), damping)
    diag, pair = pl.pallas_call(
        finish,
        out_shape=[jax.ShapeDtypeStruct((chunk, width), jnp.float32)] * 2,
        in_specs=[vmem] * 3,
        out_specs=[vmem] * 2,
    )(low, pair, carried)
    return diag.T[None], pair.T[None]


def solution(mesh):
    placed = (P(("pts", "grp"), None, None, None), P(("pts", "grp"), None), P("pts", None))
    return jax.shard_map(
        local,
        mesh=mesh,
        in_specs=placed,
        out_specs=(P("pts", None, "grp"), P("pts", None, "grp")),
        check_vma=False,
    )
```

```python
import functools

import jax
import jax.numpy as jnp
from jax import lax
from jax.experimental import pallas as pl
from jax.experimental.pallas import tpu as pltpu
from jax.sharding import PartitionSpec as P

MESH = pl.DeviceIdType.MESH
LANES = 128
TILE = 8


def mm(left, right, dims, precise):
    return lax.dot_general(
        left,
        right,
        (dims, ((), ())),
        precision=lax.Precision.HIGHEST if precise else None,
        preferred_element_type=jnp.float32,
    )


NN = ((1,), (0,))
NT = ((1,), (1,))
TN = ((0,), (0,))


def sweep_steps(matrix, rounds):
    size = matrix.shape[0]
    lane_row = lax.broadcasted_iota(jnp.int32, (1, size), 1)
    lane = lax.broadcasted_iota(jnp.int32, (size, size), 1)
    top_row = lax.broadcasted_iota(jnp.int32, (TILE, size), 0)

    def body(_, a):
        for t in range(TILE):
            row = a[t : t + 1, :]
            col = a[:, t : t + 1]
            scaled = jnp.where(lane_row == t, -1.0, row) * (1.0 / a[t : t + 1, t : t + 1])
            new = jnp.where(lane == t, 0.0, a) - col * scaled
            top = jnp.where(top_row == t, scaled, new[:TILE])
            a = jnp.concatenate([top, new[TILE:]], 0)
        a = pltpu.roll(a, size - TILE, 1)
        return jnp.concatenate([a[TILE:], a[:TILE]], 0)

    return lax.fori_loop(0, rounds, body, matrix)


def kernel(
    owners, groups, rows_per, width, capacity,
    planes, owner_row, damp, low_out, pair_out, carried,
    send, recv, sblk, s1, s2, gram, r1, r2, bt, highs,
    a_send, a_recv, d_send, d_recv, d2_recv, g_send, g_recv, b_send, b_recv, c_send, c_recv, own_sem,
):
    me = lax.axis_index("pts")
    grp = lax.axis_index("grp")
    near = grp + 1 - 2 * lax.rem(grp, 2)
    far = lax.rem(grp + 2, groups)
    chunk = width // groups
    nb = width // LANES
    pairs = [(i, j) for i in range(nb) for j in range(i, nb)]
    odd = lax.rem(grp, 2)

    barrier = pltpu.get_barrier_semaphore()

    def greet(off, _):
        pl.semaphore_signal(
            barrier, inc=1, device_id=(lax.rem(me + off, owners), grp), device_id_type=MESH
        )
        return 0

    lax.fori_loop(1, owners, greet, 0)
    for other in (near, far):
        pl.semaphore_signal(barrier, inc=1, device_id=(me, other), device_id_type=MESH)

    clusters, spots, _ = planes.shape
    points = owner_row.shape[1]
    earlier = (
        lax.broadcasted_iota(jnp.int32, (points, points), 0)
        < lax.broadcasted_iota(jnp.int32, (points, points), 1)
    )
    spread = jnp.broadcast_to(owner_row[...], (points, points))
    ahead = jnp.where((spread.T == spread) & earlier, 1, 0)
    place = owner_row[...] * rows_per + jnp.sum(ahead, axis=0, keepdims=True)
    place = jnp.concatenate([place + capacity * r for r in range(spots // points)], 1)
    slot = lax.broadcasted_iota(jnp.int32, (owners * rows_per, spots), 0)
    pick = jnp.where(slot == place, 1.0, 0.0).astype(send.dtype)

    def pack(k):
        send[k] = mm(pick, planes[k], NN, False).astype(send.dtype)

    pack(1)
    pl.semaphore_wait(barrier, owners - 1 + 2)

    def rows_at(i):
        return pl.ds(pl.multiple_of(i * rows_per, rows_per), rows_per)

    for k in (1, 0, 2):
        if k != 1:
            pack(k)

        def issue(off, _, k=k):
            to = lax.rem(me + off, owners)
            pltpu.make_async_remote_copy(
                src_ref=send.at[k, rows_at(to)],
                dst_ref=recv.at[k, rows_at(me)],
                send_sem=a_send.at[k],
                recv_sem=a_recv.at[k],
                device_id=(to, grp),
                device_id_type=MESH,
            ).start()
            return 0

        lax.fori_loop(1, owners, issue, 0)
    for k in range(3):
        pltpu.make_async_copy(
            send.at[k, rows_at(me)], recv.at[k, rows_at(me)], own_sem.at[k]
        ).start()
    for k in range(3):
        pltpu.make_async_copy(
            send.at[k, rows_at(me)], recv.at[k, rows_at(me)], own_sem.at[k]
        ).wait()

    def await_rows(k):
        part = recv.at[k, pl.ds(0, (owners - 1) * rows_per)]
        pltpu.make_async_copy(part, part, a_recv.at[k]).wait()

    await_rows(1)
    first_copies = []
    own = len(pairs)
    for i in range(nb):
        strip = mm(
            recv[1, :, i * LANES : (i + 1) * LANES], recv[1, :, i * LANES :], TN, False
        )
        for j in range(i, nb):
            n = pairs.index((i, j))
            sblk[n] = strip[:, (j - i) * LANES : (j - i + 1) * LANES]
            copy = pltpu.make_async_remote_copy(
                src_ref=sblk.at[n], dst_ref=s1.at[n],
                send_sem=d_send.at[n], recv_sem=d_recv.at[n],
                device_id=(me, near), device_id_type=MESH,
            )
            copy.start()
            first_copies.append(copy)
    second_copies = []

    def forward(some):
        for n in some:
            first_copies[n].wait_recv()
            sblk[own + n] = sblk[n] + s1[n]
            copy = pltpu.make_async_remote_copy(
                src_ref=sblk.at[own + n], dst_ref=s2.at[n],
                send_sem=d_send.at[own + n], recv_sem=d2_recv.at[n],
                device_id=(me, far), device_id_type=MESH,
            )
            copy.start()
            second_copies.append(copy)

    forward(range(1))

    eye = (
        lax.broadcasted_iota(jnp.int32, (LANES, LANES), 0)
        == lax.broadcasted_iota(jnp.int32, (LANES, LANES), 1)
    )

    def reduced(n):
        second_copies[n].wait_recv()
        i, j = pairs[n]
        total = sblk[own + n] + s2[n]
        if i == j:
            total = total + jnp.where(eye, damp[:, i * LANES : (i + 1) * LANES], 0.0)
        return total

    where_in = {pair: n for n, pair in enumerate(pairs)}
    blocks = {}
    inverses, factors = [], {}
    rounds = LANES // TILE

    sides = ((0, 1), (2, 1), (0, 0), (2, 2), (2, 0))

    def chunk_rows(c):
        return pl.ds(pl.multiple_of(c * chunk, TILE), chunk)

    def near_copy(m, h):
        return pltpu.make_async_remote_copy(
            src_ref=gram.at[m, chunk_rows(1 - odd + 2 * h)], dst_ref=r1.at[m, h],
            send_sem=g_send.at[m, h], recv_sem=g_recv.at[m, h],
            device_id=(me, near), device_id_type=MESH,
        )

    def far_copy(m, h):
        return pltpu.make_async_remote_copy(
            src_ref=gram.at[m, chunk_rows(odd + 2 * h if m < 2 else far)], dst_ref=r2.at[m, h],
            send_sem=g_send.at[m, 2 + h], recv_sem=g_recv.at[m, 2 + h],
            device_id=(me, far), device_id_type=MESH,
        )

    def spread_near(m, h):
        at = chunk_rows(odd + 2 * h)
        return pltpu.make_async_remote_copy(
            src_ref=bt.at[m, at], dst_ref=bt.at[m, at],
            send_sem=b_send.at[m, h], recv_sem=b_recv.at[m, h],
            device_id=(me, near), device_id_type=MESH,
        )

    def far_parts(m):
        return range(2) if m < 2 else range(1)

    def make_grams(k, some):
        await_rows(k)
        for m in some:
            left, right = sides[m]
            gram[m] = mm(recv[left], recv[right], TN, False)
            for h in range(2):
                near_copy(m, h).start()

    def fold_near(some):
        for m in some:
            for h in range(2):
                near_copy(m, h).wait()
                at = chunk_rows(odd + 2 * h)
                gram[m, at, :] = gram[m, at, :] + r1[m, h]
            for h in far_parts(m):
                far_copy(m, h).start()

    def fold_far(m):
        for h in far_parts(m):
            far_copy(m, h).wait()
            if m < 2:
                at = chunk_rows(odd + 2 * h)
                bt[m, at, :] = gram[m, at, :] + r2[m, h]
                spread_near(m, h).start()
            else:
                at = chunk_rows(grp)
                gram[m, at, :] = gram[m, at, :] + r2[m, h]

    def second_near():
        fold_near((1,))
        fold_far(0)

    quarters = 4
    hooks = {
        (0, 1): functools.partial(forward, range(1, own)),
        (0, quarters): functools.partial(make_grams, 0, (0, 2)),
        (1, 1): functools.partial(fold_near, (0,)),
        (1, 2): functools.partial(fold_near, (2,)),
        (1, quarters): functools.partial(make_grams, 2, (1, 3, 4)),
        (2, 1): second_near,
        (2, 2): functools.partial(fold_near, (3,)),
        (2, 3): functools.partial(fold_near, (4,)),
    }

    def block(i, j):
        if (i, j) not in blocks:
            blocks[i, j] = reduced(where_in[i, j])
        return blocks[i, j]

    for i in range(nb):
        a = block(i, i)
        for part in range(1, quarters + 1):
            a = sweep_steps(a, rounds // quarters)
            if part < quarters and (i, part) in hooks:
                hooks.pop((i, part))()
        a = -a
        inverses.append(a)
        for j in range(i + 1, nb):
            factors[i, j] = mm(a, block(i, j), NN, True)
        if (i, quarters) in hooks:
            hooks.pop((i, quarters))()
        for j in range(i + 1, nb):
            for k in range(j, nb):
                blocks[j, k] = block(j, k) - mm(block(i, j), factors[i, k], TN, True)
    for key in sorted(hooks):
        hooks[key]()
    mine = chunk_rows(grp)

    def eliminate(m):
        for h in range(2):
            spread_near(m, h).wait()
        for j in range(1, nb):
            value = bt[m, :, j * LANES : (j + 1) * LANES]
            for i in range(j):
                value = value - mm(
                    bt[m, :, i * LANES : (i + 1) * LANES], factors[i, j], NN, True
                )
            bt[m, :, j * LANES : (j + 1) * LANES] = value
        return jnp.concatenate(
            [
                mm(bt[m, mine, i * LANES : (i + 1) * LANES], inverses[i], NN, True)
                for i in range(nb)
            ],
            1,
        )

    fold_far(1)
    solved_low = eliminate(0)
    fold_far(2)
    low_out[...] = gram[2, mine, :] - mm(solved_low, bt[0], NT, True)
    solved_high = eliminate(1)
    fold_far(3)
    highs[...] = gram[3, mine, :] - mm(solved_high, bt[1], NT, True)
    carry = pltpu.make_async_remote_copy(
        src_ref=highs, dst_ref=carried, send_sem=c_send, recv_sem=c_recv,
        device_id=(lax.rem(me + 1, owners), grp), device_id_type=MESH,
    )
    carry.start()
    fold_far(4)
    pair_out[...] = gram[4, mine, :] - mm(solved_high, bt[0], NT, True)
    for copy in first_copies + second_copies:
        copy.wait_send()
    for k in range(3):
        part = send.at[k, pl.ds(0, (owners - 1) * rows_per)]
        pltpu.make_async_copy(part, part, a_send.at[k]).wait()
    carry.wait()


def finish(low, pair, carried, diag_out, pair_out):
    diag_out[...] = low[...] + carried[...]
    pair_out[...] = pair[...]


def local(jacobian, owner, damping):
    points, clusters, residuals, width = jacobian.shape
    owners = lax.axis_size("pts")
    groups = lax.axis_size("grp")
    capacity = max(2, 2 * points // owners)
    rows_per = -(-residuals * capacity // 16) * 16
    total = owners * rows_per
    planes = jnp.transpose(jacobian, (1, 2, 0, 3)).reshape(clusters, residuals * points, width)
    chunk = width // groups
    nb = width // LANES
    blocks = nb * (nb + 1) // 2
    vmem = pl.BlockSpec(memory_space=pltpu.VMEM)
    dma = pltpu.SemaphoreType.DMA
    low, pair, carried = pl.pallas_call(
        functools.partial(kernel, owners, groups, rows_per, width, capacity),
        out_shape=[jax.ShapeDtypeStruct((chunk, width), jnp.float32)] * 3,
        in_specs=[vmem] * 3,
        out_specs=[vmem] * 3,
        scratch_shapes=[
            pltpu.VMEM((clusters, total, width), jacobian.dtype),
            pltpu.VMEM((clusters, total, width), jacobian.dtype),
            pltpu.VMEM((2 * blocks, LANES, LANES), jnp.float32),
            pltpu.VMEM((blocks, LANES, LANES), jnp.float32),
            pltpu.VMEM((blocks, LANES, LANES), jnp.float32),
            pltpu.VMEM((5, width, width), jnp.float32),
            pltpu.VMEM((5, 2, chunk, width), jnp.float32),
            pltpu.VMEM((5, 2, chunk, width), jnp.float32),
            pltpu.VMEM((2, width, width), jnp.float32),
            pltpu.VMEM((chunk, width), jnp.float32),
            dma((3,)), dma((3,)),
            dma((2 * blocks,)), dma((blocks,)), dma((blocks,)),
            dma((5, 4)), dma((5, 4)),
            dma((2, 2)), dma((2, 2)),
            dma, dma, dma((3,)),
        ],
        compiler_params=pltpu.CompilerParams(collective_id=0, has_side_effects=True),
    )(planes, owner.reshape(1, points), damping)
    diag, pair = pl.pallas_call(
        finish,
        out_shape=[jax.ShapeDtypeStruct((chunk, width), jnp.float32)] * 2,
        in_specs=[vmem] * 3,
        out_specs=[vmem] * 2,
    )(low, pair, carried)
    return diag.T[None], pair.T[None]


def solution(mesh):
    placed = (P(("pts", "grp"), None, None, None), P(("pts", "grp"), None), P("pts", None))
    return jax.shard_map(
        local,
        mesh=mesh,
        in_specs=placed,
        out_specs=(P("pts", None, "grp"), P("pts", None, "grp")),
        check_vma=False,
    )
```
